32 devices in a mesh: member: 2 (over x), dp: 16 (over z, y, core).
Axes of the slice: x: 2, y: 2, z: 4, core: 2. Of those that a mesh axis runs over, the one named last changes fastest.
Arguments:
- residual: bfloat16 [512, 3072], P(('member', 'dp')), parts along dimension 0, may hold values from -6 to 6
- upstream: bfloat16 [512, 3072], P(('member', 'dp')), parts along dimension 0, may hold values from -6 to 6
- gate_weight: bfloat16 [6144, 10240], P('member', 'dp'), parts along dimension 0, may hold values from -0.109375 to 0.109375
- up_weight: bfloat16 [6144, 10240], P('member', 'dp'), parts along dimension 0, may hold values from -0.109375 to 0.109375
- down_weight: bfloat16 [20480, 3072], P(('member', 'dp')), parts along dimension 0, may hold values from -0.0625 to 0.0625
- gain: float32 [6144], P('member'), parts along dimension 0, may hold values from 0.25 to 1.75
Outputs:
- grad_residual: bfloat16 [512, 3072], P(('member', 'dp')), parts along dimension 0
- grad_gate: bfloat16 [6144, 10240], P('member', 'dp'), parts along dimension 0
- grad_up: bfloat16 [6144, 10240], P('member', 'dp'), parts along dimension 0
- grad_down: bfloat16 [20480, 3072], P(('member', 'dp')), parts along dimension 0
- grad_gain: float32 [6144], P('member'), parts along dimension 0
The draws below stay inside these ranges and needn't reach their ends.
There are 2 independent parts, one for each index of `member`. The reference program is written for one: setup_inputs(seed, part) draws one part's arguments, and reference() takes and returns one part's arrays. A program takes and returns all parts, laid end to end along the dimension named above; each array names one. Nothing has to cross between parts.
All inputs are finite; a program needn't handle non-finite values.
Results may differ from the reference program's by a relative error of at most 0.0068.
Values may be sent and summed in bfloat16 or wider, within the bound.
No kernel may reach another device: no remote copies, remote signals or barrier semaphores. Data moves between devices by JAX's collectives and lax.ppermute only.
A program may use at most 128 MiB of HBM per device.

```python
import jax
import jax.numpy as jnp
from jax import lax

D = 3072
FF = 10240
TOKENS = 256


def block_scale(stream_key, dims, pieces, smallest, high):
    level, own = 1.0, jax.random.fold_in(stream_key, 6)
    for dim, blocks in pieces:
        steps = jnp.exp(jax.random.uniform(jax.random.fold_in(own, dim), (blocks,), jnp.float32, smallest / len(pieces), high / len(pieces)))
        level = level * jnp.repeat(steps, dims[dim] // blocks).reshape([-1 if axis == dim else 1 for axis in range(len(dims))])
    return level


def normal_values(key, shape, scale, most, split=(), held_as=jnp.bfloat16):
    entries = jax.random.normal(key, shape, jnp.float32) * scale
    if len(split) > 0:
        entries = block_scale(key, shape, split, -0.22, 0.18) * entries
    return jnp.clip(entries, min=-most, max=most).astype(held_as)


def setup_inputs(seed: int = 0, part: int = 0) -> dict:
    key_of = jax.random.split(jax.random.key(seed), 7)
    own_keys = jax.random.split(jax.random.fold_in(key_of[6], part), 7)
    return {
        "residual": normal_values(own_keys[0], (TOKENS, D), 1.0, 6.0, ((0, 16),)),
        "upstream": normal_values(own_keys[1], (TOKENS, D), 1.0, 6.0, ((0, 16),)),
        "gate_weight": normal_values(own_keys[2], (D, FF), D ** -0.5, 0.109375, ((1, 16),)),
        "up_weight": normal_values(own_keys[3], (D, FF), D ** -0.5, 0.109375, ((1, 16),)),
        "down_weight": normal_values(own_keys[4], (FF, D), FF ** -0.5, 0.0625, ((0, 16),)),
        "gain": jnp.clip(1.0 + 0.15 * jax.random.normal(own_keys[5], (D,), jnp.float32), 0.25, 1.75),
    }


norm_floor = 0.5
gelu_coeff = 0.7978845608
cubic_term = 0.044715

def gelu_parts(gate_out):
    inner = jnp.tanh(gelu_coeff * (gate_out + cubic_term * gate_out * gate_out * gate_out))
    activated = 0.5 * gate_out * (1.0 + inner)
    gelu_slope = 0.5 * (1.0 + inner) + 0.5 * gate_out * (1.0 - inner * inner) * gelu_coeff * (1.0 + 3.0 * cubic_term * gate_out * gate_out)
    return (activated, gelu_slope)

def contract_last(left, right):
    return lax.dot_general(left, right, (((1,), (1,)), ((), ())), preferred_element_type=jnp.float32)

def contract_first(left, right):
    return lax.dot_general(left, right, (((0,), (0,)), ((), ())), preferred_element_type=jnp.float32)

def reference(residual, upstream, gate_weight, up_weight, down_weight, gain):
    widened = residual.astype(jnp.float32)
    norm_scale = lax.rsqrt(lax.optimization_barrier(jnp.mean(widened * widened, axis=1, keepdims=True)) + norm_floor)
    unit_rows = widened * norm_scale
    normed = (unit_rows * gain).astype(jnp.bfloat16)
    gate_out = jnp.dot(normed, gate_weight, preferred_element_type=jnp.float32)
    up_out = jnp.dot(normed, up_weight, preferred_element_type=jnp.float32)
    activated, gelu_slope = gelu_parts(gate_out)
    hidden = (activated * up_out).astype(jnp.bfloat16)
    hidden_grad = contract_last(upstream, down_weight)
    grad_down = contract_first(hidden, upstream).astype(jnp.bfloat16)
    gate_grad = (hidden_grad * up_out * gelu_slope).astype(jnp.bfloat16)
    up_grad = (hidden_grad * activated).astype(jnp.bfloat16)
    grad_gate = contract_first(normed, gate_grad).astype(jnp.bfloat16)
    grad_up = contract_first(normed, up_grad).astype(jnp.bfloat16)
    normed_grad = contract_last(gate_grad, gate_weight) + contract_last(up_grad, up_weight)
    unit_grad = normed_grad * gain
    inner_mean = lax.optimization_barrier(jnp.mean(unit_grad * unit_rows, axis=1, keepdims=True))
    grad_residual = (upstream.astype(jnp.float32) + norm_scale * (unit_grad - unit_rows * inner_mean)).astype(jnp.bfloat16)
    grad_gain = lax.optimization_barrier(jnp.sum(normed_grad * unit_rows, axis=0))
    return (grad_residual, grad_gate, grad_up, grad_down, grad_gain)
```

```python
import jax
import jax.numpy as jnp
from jax import lax
from jax.sharding import PartitionSpec as P

norm_floor = 0.5
gelu_coeff = 0.7978845608
cubic_term = 0.044715


def gelu_parts(gate_out):
    inner = jnp.tanh(gelu_coeff * (gate_out + cubic_term * gate_out * gate_out * gate_out))
    activated = 0.5 * gate_out * (1.0 + inner)
    gelu_slope = 0.5 * (1.0 + inner) + 0.5 * gate_out * (1.0 - inner * inner) * gelu_coeff * (
        1.0 + 3.0 * cubic_term * gate_out * gate_out
    )
    return (activated, gelu_slope)


def contract_last(left, right):
    return lax.dot_general(
        left, right, (((1,), (1,)), ((), ())), preferred_element_type=jnp.float32
    )


def contract_first(left, right):
    return lax.dot_general(
        left, right, (((0,), (0,)), ((), ())), preferred_element_type=jnp.float32
    )


class Chips:
    def __init__(self, size):
        self.count = size // 2
        ids = list(range(self.count))
        self.ring = ids[0::2] + ids[1::2][::-1]

    def hop(self, values, distance):
        pairs = []
        for place, chip in enumerate(self.ring):
            target = self.ring[(place + distance) % self.count]
            pairs += [(2 * chip + core, 2 * target + core) for core in range(2)]
        return lax.ppermute(values, "dp", pairs)

    def swap(self, values):
        return lax.ppermute(values, "dp", [(i, i ^ 1) for i in range(2 * self.count)])

    def gather(self, values):
        width = values.shape[1]
        behind, ahead = [values], [values]
        for _ in range((self.count - 1) // 2):
            behind.append(self.hop(behind[-1], 1))
            ahead.append(self.hop(ahead[-1], -1))
        blocks = behind + ahead[1:]
        if self.count % 2 == 0:
            left = self.hop(behind[-1][:, : width // 2], 1)
            right = self.hop(ahead[-1][:, width // 2 :], -1)
            blocks.append(jnp.concatenate([left, right], axis=1))
        return blocks

    def offsets(self):
        reach = (self.count - 1) // 2
        order = [0] + [-s for s in range(1, reach + 1)] + list(range(1, reach + 1))
        return order + ([self.count // 2] if self.count % 2 == 0 else [])


def make_per_device(size):
    chips = Chips(size)

    def per_device(residual, upstream, gate_weight, up_weight, down_weight, gain):
        tokens, width = residual.shape
        mine = jnp.concatenate(chips.gather(jnp.concatenate([residual, upstream], axis=1)), axis=0)
        rows = jnp.concatenate([mine, chips.swap(mine)], axis=0)
        half = mine.shape[0]

        widened = rows[:, :width].astype(jnp.float32)
        upstream_all = rows[:, width:]
        norm_scale = lax.rsqrt(jnp.mean(widened * widened, axis=1, keepdims=True) + norm_floor)
        unit_rows = widened * norm_scale
        normed_all = (unit_rows * gain).astype(jnp.bfloat16)

        gate_out = jnp.dot(normed_all, gate_weight, preferred_element_type=jnp.float32)
        up_out = jnp.dot(normed_all, up_weight, preferred_element_type=jnp.float32)
        activated, gelu_slope = gelu_parts(gate_out)
        hidden = (activated * up_out).astype(jnp.bfloat16)
        hidden_grad = contract_last(upstream_all, down_weight)
        gate_grad = (hidden_grad * up_out * gelu_slope).astype(jnp.bfloat16)
        up_grad = (hidden_grad * activated).astype(jnp.bfloat16)
        partial_grad = contract_last(gate_grad, gate_weight) + contract_last(up_grad, up_weight)

        gain_part = jnp.sum(partial_grad * unit_rows, axis=0).reshape(tokens, width // tokens)
        gain_high = gain_part.astype(jnp.bfloat16)
        gain_low = (gain_part - gain_high.astype(jnp.float32)).astype(jnp.bfloat16)
        gain_terms = jnp.concatenate([gain_high, gain_low], axis=1)
        given, gain_given = chips.swap((partial_grad[half:].astype(jnp.bfloat16), gain_terms))
        pair_grad = partial_grad[:half] + given.astype(jnp.float32)
        share = width // tokens

        def terms_sum(terms):
            terms = terms.astype(jnp.float32)
            return terms[:, :share] + terms[:, share:]

        gain_pair = gain_part + terms_sum(gain_given)
        pair_high = gain_pair.astype(jnp.bfloat16)
        pair_low = (gain_pair - pair_high.astype(jnp.float32)).astype(jnp.bfloat16)
        sent = pair_grad.astype(jnp.bfloat16)
        normed_grad = pair_grad[:tokens]
        gain_sum = gain_pair
        for index, offset in sorted(enumerate(chips.offsets()), key=lambda item: -abs(item[1])):
            if offset == 0:
                continue
            block = jnp.concatenate(
                [sent[index * tokens : (index + 1) * tokens], pair_high, pair_low], axis=1
            )
            came = chips.hop(block, offset)
            normed_grad = normed_grad + came[:, :width].astype(jnp.float32)
            gain_sum = gain_sum + terms_sum(came[:, width:])

        grad_down = contract_first(hidden, upstream_all).astype(jnp.bfloat16)
        grad_gate = contract_first(normed_all, gate_grad).astype(jnp.bfloat16)
        grad_up = contract_first(normed_all, up_grad).astype(jnp.bfloat16)

        own_rows = unit_rows[:tokens]
        unit_grad = normed_grad * gain
        inner_mean = jnp.mean(unit_grad * own_rows, axis=1, keepdims=True)
        grad_residual = (
            upstream.astype(jnp.float32)
            + norm_scale[:tokens] * (unit_grad - own_rows * inner_mean)
        ).astype(jnp.bfloat16)
        return (grad_residual, grad_gate, grad_up, grad_down, gain_sum.reshape(width))

    return per_device


def solution(mesh):
    placed = (
        P(("member", "dp"), None),
        P(("member", "dp"), None),
        P("member", "dp"),
        P("member", "dp"),
        P(("member", "dp"), None),
        P("member"),
    )
    return jax.shard_map(
        make_per_device(mesh.shape["dp"]),
        mesh=mesh,
        in_specs=placed,
        out_specs=(
            P(("member", "dp"), None),
            P("member", "dp"),
            P("member", "dp"),
            P(("member", "dp"), None),
            P("member"),
        ),
        check_vma=False,
    )
```
